32 devices in a mesh: gx: 2 (over x), gy: 4 (over z), gz: 4 (over y, core).
Axes of the slice: x: 2, y: 2, z: 4, core: 2. Of those that a mesh axis runs over, the one named last changes fastest.
Arguments:
- populations: float32 [39, 16, 96, 512], P(None, 'gx', 'gy', 'gz'), may hold values from 0.5 to 1.5
- relax: float32 [16, 96, 512], P('gx', 'gy', 'gz'), may hold values from 0.6 to 1.9
Outputs:
- advanced: float32 [39, 16, 96, 512], P(None, 'gx', 'gy', 'gz')
The draws below stay inside these ranges and needn't reach their ends.
All inputs are finite; a program needn't handle non-finite values.
Results may differ from the reference program's by a relative error of at most 0.0001.
Values sent between devices are 32-bit elements; how exact they have to be, the bound alone decides.
A program may use at most 128 MiB of HBM per device.

```python
import math
import jax
import jax.numpy as jnp

Q = 39
STEPS = 1
NX = 16
NY = 96
NZ = 512


def steps_of(stream_key, shape, cuts, least, high):
    level, own = 1.0, jax.random.fold_in(stream_key, 6)
    for position, blocks in cuts:
        heights = jnp.exp(jax.random.uniform(jax.random.fold_in(own, position), (blocks,), jnp.float32, least / len(cuts), high / len(cuts)))
        level = level * jnp.repeat(heights, shape[position] // blocks).reshape([-1 if axis == position else 1 for axis in range(len(shape))])
    return level


def setup_inputs(seed: int = 0) -> dict:
    splits = jax.random.split(jax.random.key(seed), 3)
    return {
        "populations": jnp.clip(0.5 + 1.0 * jax.random.uniform(splits[0], (Q, NX, NY, NZ), jnp.float32) ** steps_of(splits[0], (Q, NX, NY, NZ), ((1, 2), (2, 4), (3, 4)), -0.2, 0.2), 0.5, 1.5),
        "relax": jnp.clip(jnp.exp(math.log(1.9) - 1.1526795 * jax.random.uniform(splits[1], (NX, NY, NZ), jnp.float32) ** steps_of(splits[1], (NX, NY, NZ), ((0, 2), (1, 4), (2, 4)), -0.2, 0.2)), 0.6, 1.9),
    }


def lattice():
    speeds = [(0, 0, 0)]
    weights = [1.0 / 12.0]
    for axis in range(3):
        for sign in (1, -1):
            vector = [0, 0, 0]
            vector[axis] = sign
            speeds.append(tuple(vector))
            weights.append(1.0 / 12.0)
    for first in (1, -1):
        for second in (1, -1):
            for third in (1, -1):
                speeds.append((first, second, third))
                weights.append(1.0 / 27.0)
    for axis in range(3):
        for sign in (2, -2):
            vector = [0, 0, 0]
            vector[axis] = sign
            speeds.append(tuple(vector))
            weights.append(2.0 / 135.0)
    for couple in ((0, 1), (0, 2), (1, 2)):
        for first in (2, -2):
            for second in (2, -2):
                vector = [0, 0, 0]
                vector[couple[0]] = first
                vector[couple[1]] = second
                speeds.append(tuple(vector))
                weights.append(1.0 / 432.0)
    for axis in range(3):
        for sign in (3, -3):
            vector = [0, 0, 0]
            vector[axis] = sign
            speeds.append(tuple(vector))
            weights.append(1.0 / 1620.0)
    return speeds, weights


def collide(popul, rate):
    speeds, weights = lattice()
    acoustic_wave_rate = 2.0 / 3.0
    inverse = 1.0 / (acoustic_wave_rate ** 0.5)
    zeroth_moment_rho = sum(weights[member] * popul[member] for member in range(39))
    flux = [sum(weights[member] * speeds[member][axis] * popul[member] for member in range(39) if speeds[member][axis] != 0) for axis in range(3)]
    thermal_heat_content = sum(weights[member] * float(sum(value * value for value in speeds[member])) * popul[member] for member in range(1, 39))
    velocity = [part / zeroth_moment_rho for part in flux]
    flow_norm_square = velocity[0] * velocity[0] + velocity[1] * velocity[1] + velocity[2] * velocity[2]
    site_kinetic_heat = (thermal_heat_content / zeroth_moment_rho - flow_norm_square) / (3.0 * acoustic_wave_rate)
    scaled = [part * inverse for part in velocity]
    scaled_square = flow_norm_square / acoustic_wave_rate
    excess_quantity = site_kinetic_heat - 1.0
    results = []
    for member in range(39):
        vector = speeds[member]
        aligned = sum(vector[axis] * inverse * scaled[axis] for axis in range(3) if vector[axis] != 0) if member > 0 else jnp.zeros_like(zeroth_moment_rho)
        speed_square = float(sum(value * value for value in vector)) / acoustic_wave_rate
        aligned_square = aligned * aligned
        hermite = (1.0 + aligned
                   + 0.5 * (aligned_square - scaled_square + excess_quantity * (speed_square - 3.0))
                   + aligned * (aligned_square - 3.0 * scaled_square + 3.0 * excess_quantity * (speed_square - 5.0)) / 6.0
                   + (aligned_square * aligned_square - 6.0 * aligned_square * scaled_square + 3.0 * scaled_square * scaled_square
                      + 6.0 * excess_quantity * (aligned_square * (speed_square - 7.0) + scaled_square * (5.0 - speed_square))
                      + 3.0 * excess_quantity * excess_quantity * (speed_square * speed_square - 10.0 * speed_square + 15.0)) / 24.0)
        maxwellian_target = zeroth_moment_rho * hermite
        results.append(popul[member] - rate * (popul[member] - maxwellian_target))
    return jnp.stack(results)


def reference(populations, relax):
    speeds, weights = lattice()
    state = populations
    for number in range(STEPS):
        post = collide(state, relax)
        state = jnp.stack([jnp.roll(post[member], speeds[member], axis=(0, 1, 2)) for member in range(39)])
    return state
```

```python
import functools

import jax
import jax.numpy as jnp
from jax import lax
from jax.experimental import pallas as pl
from jax.experimental.pallas import tpu as pltpu
from jax.sharding import PartitionSpec as P

MESH = pl.DeviceIdType.MESH
AXES = ("gx", "gy", "gz")
PX = 3
PY = 8
GROUP = 32


def lattice():
    speeds = [(0, 0, 0)]
    weights = [1.0 / 12.0]
    for axis in range(3):
        for sign in (1, -1):
            vector = [0, 0, 0]
            vector[axis] = sign
            speeds.append(tuple(vector))
            weights.append(1.0 / 12.0)
    for first in (1, -1):
        for second in (1, -1):
            for third in (1, -1):
                speeds.append((first, second, third))
                weights.append(1.0 / 27.0)
    for axis in range(3):
        for sign in (2, -2):
            vector = [0, 0, 0]
            vector[axis] = sign
            speeds.append(tuple(vector))
            weights.append(2.0 / 135.0)
    for couple in ((0, 1), (0, 2), (1, 2)):
        for first in (2, -2):
            for second in (2, -2):
                vector = [0, 0, 0]
                vector[couple[0]] = first
                vector[couple[1]] = second
                speeds.append(tuple(vector))
                weights.append(1.0 / 432.0)
    for axis in range(3):
        for sign in (3, -3):
            vector = [0, 0, 0]
            vector[axis] = sign
            speeds.append(tuple(vector))
            weights.append(1.0 / 1620.0)
    return (speeds, weights)


SPEEDS, WEIGHTS = lattice()
Q = len(SPEEDS)
SQUARES = [sum(v * v for v in c) for c in SPEEDS]
PAIRS = [
    (m, SPEEDS.index(tuple(-v for v in SPEEDS[m])))
    for m in range(1, Q)
    if m < SPEEDS.index(tuple(-v for v in SPEEDS[m]))
]


def offsets(axis, sign, keep):
    rows, start = [], 0
    for m, c in enumerate(SPEEDS):
        count = c[axis] * sign
        if count > 0 and keep(c):
            rows.append((m, start, count))
            start += count
    return rows


ZCOLS = [offsets(2, sign, lambda c: True) for sign in (1, -1)]
Y1ROWS = [offsets(1, sign, lambda c: c[2] == 0) for sign in (1, -1)]
Y2ROWS = [offsets(1, sign, lambda c: c[2] != 0) for sign in (1, -1)]
Y1SIZE, Y2SIZE = 16, 8

XPURE = [[(SPEEDS.index((s * k, 0, 0)), 1, k) for s in (1, -1)] for k in (1, 2, 3)]
XZ = [(SPEEDS.index((s * 2, 0, 2)), 2, 2) for s in (1, -1)]
XY = [(SPEEDS.index((s * 2, 2, 0)), 2, 2) for s in (1, -1)]
XYZ = [(SPEEDS.index((s, 1, 1)), 4, 1) for s in (1, -1)]


def add_all(terms):
    total = terms[0]
    for term in terms[1:]:
        total = total + term
    return total


def collide(load, rate, emit):
    sums = {k: [] for k in (1, 3, 4, 8, 9)}
    flows = {k: [[], [], []] for k in (1, 3, 4, 8, 9)}
    for m, o in PAIRS:
        up, down = load(m), load(o)
        k = SQUARES[m]
        sums[k].append(up + down)
        diff = up - down
        for axis in range(3):
            if SPEEDS[m][axis] > 0:
                flows[k][axis].append((1, diff))
            elif SPEEDS[m][axis] < 0:
                flows[k][axis].append((-1, diff))
    weight = {SQUARES[m]: WEIGHTS[m] for m in range(Q)}
    size = {1: 1, 3: 1, 4: 2, 8: 2, 9: 3}
    rest = load(0)
    groups = {k: add_all(sums[k]) for k in sums}
    rho = weight[0] * rest
    energy = None
    for k in sums:
        part = weight[k] * groups[k]
        rho = rho + part
        part = part if k == 1 else float(k) * part
        energy = part if energy is None else energy + part
    flux = []
    for axis in range(3):
        total = None
        for k in flows:
            part = None
            for sign, diff in flows[k][axis]:
                if part is None:
                    part = diff if sign > 0 else -diff
                else:
                    part = part + diff if sign > 0 else part - diff
            part = (weight[k] * size[k]) * part
            total = part if total is None else total + part
        flux.append(total)
    inverse = 1.0 / rho
    velocity = [part * inverse for part in flux]
    norm = velocity[0] * velocity[0] + velocity[1] * velocity[1] + velocity[2] * velocity[2]
    t = (energy * inverse - norm) * 0.5 - 1.0
    b = 1.5 * norm
    w = [1.5 * part for part in velocity]
    keep = 1.0 - rate
    k0 = rho * rate
    k24 = k0 * (1.0 / 24.0)
    k6 = k0 * (1.0 / 6.0)
    half_b = 0.5 * b
    kt = k0 * t
    ktb = kt * b
    ktt = kt * t
    base = k0 * (1.0 - half_b + 0.5 * half_b * half_b)
    base1 = k0 * (0.5 - 0.5 * half_b)
    baseo = k0 * (1.0 - half_b)

    def even0(s):
        return (
            base
            + kt * (0.5 * (s - 3.0))
            + ktb * (0.25 * (5.0 - s))
            + ktt * ((s * s - 10.0 * s + 15.0) / 8.0)
        )

    emit(0, keep * rest + even0(0.0))
    for k in sums:
        s = 1.5 * k
        e0 = even0(s)
        e1 = base1 + kt * (0.25 * (s - 7.0))
        o1 = baseo + kt * (0.5 * (s - 5.0))
        for m, o in PAIRS:
            if SQUARES[m] != k:
                continue
            a = None
            for axis in range(3):
                v = SPEEDS[m][axis]
                if v == 0:
                    continue
                unit = w[axis]
                if a is None:
                    a = unit if v > 0 else -unit
                else:
                    a = a + unit if v > 0 else a - unit
            if size[k] != 1:
                a = float(size[k]) * a
            q = a * a
            even = e0 + q * (e1 + q * k24)
            odd = a * (o1 + q * k6)
            emit(m, keep * load(m) + (even + odd))
            emit(o, keep * load(o) + (even - odd))


def kernel(
    pop, rate, ext, g, r, zs, zr, y1s, y1r, y2s, y2r,
    in_sem, z_ss, z_rs, y1_ss, y1_rs, y2_ss, y2_rs, x_ss, x_rs,
):
    nx, ny, nz = pop.shape[1:]
    inner = nx - 4
    groups = [(0, 2), (nx - 2, 2), (2, inner)]
    loads = [
        pltpu.make_async_copy(
            pop.at[:, pl.ds(first, count)], g.at[:, pl.ds(first, count)], in_sem.at[n]
        )
        for n, (first, count) in enumerate(groups)
    ]
    loads.append(pltpu.make_async_copy(rate, r, in_sem.at[3]))
    for n in (3, 0, 1, 2):
        loads[n].start()

    around = []
    for axis in AXES:
        n = lax.axis_size(axis)
        me = lax.axis_index(axis)
        around.append(({axis: lax.rem(me + 1, n)}, {axis: lax.rem(me + n - 1, n)}))
    barrier = pltpu.get_barrier_semaphore()
    for pair in around:
        for target in pair:
            pl.semaphore_signal(barrier, inc=1, device_id=target, device_id_type=MESH)

    lane = lax.broadcasted_iota(jnp.int32, (ny, nz), 1)

    def layer_a(j):
        return j + (j // 2) * (nx - 4)

    def layer_b(j):
        return j + 2

    def rows_at(m):
        start = PY + SPEEDS[m][1]
        return pl.ds(start, ny)

    def edge_rows(sign, count):
        return pl.ds(PY + ny, count) if sign == 0 else pl.ds(PY - count, count)

    def home_rows(sign, count):
        return pl.ds(PY, count) if sign == 0 else pl.ds(PY + ny - count, count)

    def collide_chunk(chunk, layer, steps):
        def step(j, packed):
            x = layer(j)
            packed = list(packed)
            mine = [jnp.zeros((ny, nz), jnp.float32), jnp.zeros((ny, nz), jnp.float32)]
            slot = [{m: (s, c) for m, s, c in ZCOLS[d]} for d in (0, 1)]

            def emit(m, value):
                cx, cy, cz = SPEEDS[m]
                if cz:
                    d = 0 if cz > 0 else 1
                    start, count = slot[d][m]
                    shift = start + count if d == 0 else start
                    moved = pltpu.roll(value, shift, 1) if shift else value
                    mask = (lane >= start) & (lane < start + count)
                    mine[d] = jnp.where(mask, moved, mine[d])
                    value = pltpu.roll(value, cz % nz, 1)
                ext[m, PX + x + cx, rows_at(m), :] = value

            collide(lambda m: g[m, x], r[x], emit)
            for d in (0, 1):
                moved = pltpu.roll(mine[d], GROUP * j, 1)
                mask = (lane >= GROUP * j) & (lane < GROUP * j + GROUP)
                packed[d] = jnp.where(mask, moved, packed[d])
            for d in (0, 1):
                for m, start, count in Y1ROWS[d]:
                    y1s[chunk, d, j, pl.ds(start, count), :] = ext[
                        m, PX + x + SPEEDS[m][0], edge_rows(d, count), :
                    ]
            return tuple(packed)

        blank = jnp.zeros((ny, nz), jnp.float32)
        packed = lax.fori_loop(0, steps, step, (blank, blank))
        for d in (0, 1):
            zs[chunk, d] = packed[d]

    def settle_z(chunk, layer, steps):
        def step(j, carry):
            x = layer(j)
            for d in (0, 1):
                back = lax.rem(nz - GROUP * j, nz)
                base = pltpu.roll(zr[chunk, d], back, 1)
                for m, start, count in ZCOLS[d]:
                    shift = start if d == 0 else start + count
                    moved = pltpu.roll(base, nz - shift, 1) if shift else base
                    mask = lane < count if d == 0 else lane >= nz - count
                    where = (m, PX + x + SPEEDS[m][0], rows_at(m), slice(None))
                    ext[where] = jnp.where(mask, moved, ext[where])
            for d in (0, 1):
                for m, start, count in Y2ROWS[d]:
                    y2s[chunk, d, j, pl.ds(start, count), :] = ext[
                        m, PX + x + SPEEDS[m][0], edge_rows(d, count), :
                    ]
            return carry

        lax.fori_loop(0, steps, step, 0)

    def settle_y(chunk, layer, steps, table, received):
        def step(j, carry):
            x = layer(j)
            for d in (0, 1):
                for m, start, count in table[d]:
                    ext[m, PX + x + SPEEDS[m][0], home_rows(d, count), :] = received[
                        chunk, d, j, pl.ds(start, count), :
                    ]
            return carry

        lax.fori_loop(0, steps, step, 0)

    def send_all(axis, chunk, src, dst, ss, rs):
        copies = []
        for d in (0, 1):
            copies.append(
                pltpu.make_async_remote_copy(
                    src_ref=src.at[chunk, d],
                    dst_ref=dst.at[chunk, d],
                    send_sem=ss.at[chunk, d],
                    recv_sem=rs.at[chunk, d],
                    device_id=around[axis][d],
                    device_id_type=MESH,
                )
            )
        for copy in copies:
            copy.start()
        return copies

    xs = []

    def send_x(pair):
        for d in (0, 1):
            first, members, layers = pair[d]
            n = len(xs)
            out_at = PX + nx if d == 0 else PX - layers
            in_at = PX if d == 0 else PX + nx - layers
            which, rows = pl.ds(first, members), pl.ds(PY, ny)
            copy = pltpu.make_async_remote_copy(
                src_ref=ext.at[which, pl.ds(out_at, layers), rows],
                dst_ref=ext.at[which, pl.ds(in_at, layers), rows],
                send_sem=x_ss.at[n],
                recv_sem=x_rs.at[n],
                device_id=around[0][d],
                device_id_type=MESH,
            )
            copy.start()
            xs.append(copy)

    for n in (3, 0, 1):
        loads[n].wait()
    collide_chunk(0, layer_a, 4)
    pl.semaphore_wait(barrier, 6)
    z_a = send_all(2, 0, zs, zr, z_ss, z_rs)
    y1_a = send_all(1, 0, y1s, y1r, y1_ss, y1_rs)
    send_x(XPURE[0])
    send_x(XPURE[1])
    loads[2].wait()
    collide_chunk(1, layer_b, inner)
    z_b = send_all(2, 1, zs, zr, z_ss, z_rs)
    y1_b = send_all(1, 1, y1s, y1r, y1_ss, y1_rs)
    send_x(XPURE[2])

    for copy in z_a:
        copy.wait_recv()
    settle_z(0, layer_a, 4)
    y2_a = send_all(1, 0, y2s, y2r, y2_ss, y2_rs)
    send_x(XZ)
    for copy in y1_a:
        copy.wait_recv()
    settle_y(0, layer_a, 4, Y1ROWS, y1r)
    send_x(XY)
    for copy in z_b:
        copy.wait_recv()
    settle_z(1, layer_b, inner)
    y2_b = send_all(1, 1, y2s, y2r, y2_ss, y2_rs)
    for copy in y2_a:
        copy.wait_recv()
    settle_y(0, layer_a, 4, Y2ROWS, y2r)
    send_x(XYZ)
    for copy in y1_b:
        copy.wait_recv()
    settle_y(1, layer_b, inner, Y1ROWS, y1r)
    for copy in y2_b:
        copy.wait_recv()
    settle_y(1, layer_b, inner, Y2ROWS, y2r)
    for copy in xs:
        copy.wait_recv()
    for copy in z_a + z_b + y1_a + y1_b + y2_a + y2_b + xs:
        copy.wait_send()


def crop(ext, out, sem):
    nx, ny = out.shape[1:3]
    parts = 3
    share = Q // parts
    copies = [
        pltpu.make_async_copy(
            ext.at[pl.ds(n * share, share), pl.ds(PX, nx), pl.ds(PY, ny)],
            out.at[pl.ds(n * share, share)],
            sem.at[n],
        )
        for n in range(parts)
    ]
    for copy in copies:
        copy.start()
    for copy in copies:
        copy.wait()


def per_device(populations, relax):
    nx, ny, nz = relax.shape
    steps = max(4, nx - 4)
    shape = (Q, nx + 2 * PX, ny + 2 * PY, nz)
    f32 = jnp.float32
    dma = pltpu.SemaphoreType.DMA
    any_space = pl.BlockSpec(memory_space=pl.ANY)
    ext = pl.pallas_call(
        kernel,
        out_shape=pltpu.VMEM(shape, f32),
        in_specs=[any_space, any_space],
        out_specs=pl.BlockSpec(memory_space=pltpu.VMEM),
        scratch_shapes=[
            pltpu.VMEM((Q, nx, ny, nz), f32),
            pltpu.VMEM((nx, ny, nz), f32),
            pltpu.VMEM((2, 2, ny, nz), f32),
            pltpu.VMEM((2, 2, ny, nz), f32),
            pltpu.VMEM((2, 2, steps, Y1SIZE, nz), f32),
            pltpu.VMEM((2, 2, steps, Y1SIZE, nz), f32),
            pltpu.VMEM((2, 2, steps, Y2SIZE, nz), f32),
            pltpu.VMEM((2, 2, steps, Y2SIZE, nz), f32),
            dma((4,)),
            dma((2, 2)), dma((2, 2)),
            dma((2, 2)), dma((2, 2)),
            dma((2, 2)), dma((2, 2)),
            dma((12,)), dma((12,)),
        ],
        compiler_params=pltpu.CompilerParams(
            collective_id=0, has_side_effects=True, vmem_limit_bytes=40 * 2**20
        ),
    )(populations, relax)
    return pl.pallas_call(
        crop,
        out_shape=jax.ShapeDtypeStruct((Q, nx, ny, nz), f32),
        in_specs=[pl.BlockSpec(memory_space=pltpu.VMEM)],
        out_specs=any_space,
        scratch_shapes=[dma((3,))],
    )(ext)


def solution(mesh):
    return jax.shard_map(
        per_device,
        mesh=mesh,
        in_specs=(P(None, "gx", "gy", "gz"), P("gx", "gy", "gz")),
        out_specs=P(None, "gx", "gy", "gz"),
        check_vma=False,
    )
```

```python
import math

import jax
import jax.numpy as jnp
from jax import lax
from jax.experimental import pallas as pl
from jax.experimental.pallas import tpu as pltpu
from jax.sharding import PartitionSpec as P

MESH = pl.DeviceIdType.MESH
AXES = ("gx", "gy", "gz")
PX = 3
PY = 8
GROUP = 32


def lattice():
    speeds = [(0, 0, 0)]
    weights = [1.0 / 12.0]
    for axis in range(3):
        for sign in (1, -1):
            vector = [0, 0, 0]
            vector[axis] = sign
            speeds.append(tuple(vector))
            weights.append(1.0 / 12.0)
    for first in (1, -1):
        for second in (1, -1):
            for third in (1, -1):
                speeds.append((first, second, third))
                weights.append(1.0 / 27.0)
    for axis in range(3):
        for sign in (2, -2):
            vector = [0, 0, 0]
            vector[axis] = sign
            speeds.append(tuple(vector))
            weights.append(2.0 / 135.0)
    for couple in ((0, 1), (0, 2), (1, 2)):
        for first in (2, -2):
            for second in (2, -2):
                vector = [0, 0, 0]
                vector[couple[0]] = first
                vector[couple[1]] = second
                speeds.append(tuple(vector))
                weights.append(1.0 / 432.0)
    for axis in range(3):
        for sign in (3, -3):
            vector = [0, 0, 0]
            vector[axis] = sign
            speeds.append(tuple(vector))
            weights.append(1.0 / 1620.0)
    return (speeds, weights)


SPEEDS, WEIGHTS = lattice()
Q = len(SPEEDS)
SQUARES = [sum(v * v for v in c) for c in SPEEDS]
PAIRS = [
    (m, SPEEDS.index(tuple(-v for v in SPEEDS[m])))
    for m in range(1, Q)
    if m < SPEEDS.index(tuple(-v for v in SPEEDS[m]))
]


def offsets(axis, sign, keep):
    rows, start = [], 0
    for m, c in enumerate(SPEEDS):
        count = c[axis] * sign
        if count > 0 and keep(c):
            rows.append((m, start, count))
            start += count
    return rows


ZCOLS = [offsets(2, sign, lambda c: True) for sign in (1, -1)]
Y1ROWS = [offsets(1, sign, lambda c: c[2] == 0) for sign in (1, -1)]
Y2ROWS = [offsets(1, sign, lambda c: c[2] != 0) for sign in (1, -1)]
Y1SIZE, Y2SIZE = 16, 8

XPURE = [[(SPEEDS.index((s * k, 0, 0)), 1, k) for s in (1, -1)] for k in (1, 2, 3)]
XZ = [(SPEEDS.index((s * 2, 0, 2)), 2, 2) for s in (1, -1)]
XY = [(SPEEDS.index((s * 2, 2, 0)), 2, 2) for s in (1, -1)]
XYZ = [(SPEEDS.index((s, 1, 1)), 4, 1) for s in (1, -1)]


def add_all(terms):
    total = terms[0]
    for term in terms[1:]:
        total = total + term
    return total


def collide(load, rate, emit):
    sums = {k: [] for k in (1, 3, 4, 8, 9)}
    flows = {k: [[], [], []] for k in (1, 3, 4, 8, 9)}
    for m, o in PAIRS:
        up, down = load(m), load(o)
        k = SQUARES[m]
        sums[k].append(up + down)
        diff = up - down
        for axis in range(3):
            if SPEEDS[m][axis] > 0:
                flows[k][axis].append((1, diff))
            elif SPEEDS[m][axis] < 0:
                flows[k][axis].append((-1, diff))
    weight = {SQUARES[m]: WEIGHTS[m] for m in range(Q)}
    size = {1: 1, 3: 1, 4: 2, 8: 2, 9: 3}
    rest = load(0)
    groups = {k: add_all(sums[k]) for k in sums}
    rho = weight[0] * rest
    energy = None
    for k in sums:
        part = weight[k] * groups[k]
        rho = rho + part
        part = part if k == 1 else float(k) * part
        energy = part if energy is None else energy + part
    flux = []
    for axis in range(3):
        total = None
        for k in flows:
            part = None
            for sign, diff in flows[k][axis]:
                if part is None:
                    part = diff if sign > 0 else -diff
                else:
                    part = part + diff if sign > 0 else part - diff
            part = (weight[k] * size[k]) * part
            total = part if total is None else total + part
        flux.append(total)
    inverse = 1.0 / rho
    velocity = [part * inverse for part in flux]
    norm = velocity[0] * velocity[0] + velocity[1] * velocity[1] + velocity[2] * velocity[2]
    t = (energy * inverse - norm) * 0.5 - 1.0
    b = 1.5 * norm
    w = [1.5 * part for part in velocity]
    keep = 1.0 - rate
    k0 = rho * rate
    k24 = k0 * (1.0 / 24.0)
    k6 = k0 * (1.0 / 6.0)
    half_b = 0.5 * b
    kt = k0 * t
    ktb = kt * b
    ktt = kt * t
    base = k0 * (1.0 - half_b + 0.5 * half_b * half_b)
    base1 = k0 * (0.5 - 0.5 * half_b)
    baseo = k0 * (1.0 - half_b)

    def even0(s):
        return (
            base
            + kt * (0.5 * (s - 3.0))
            + ktb * (0.25 * (5.0 - s))
            + ktt * ((s * s - 10.0 * s + 15.0) / 8.0)
        )

    emit(0, keep * rest + even0(0.0))
    for k in sums:
        s = 1.5 * k
        e0 = even0(s)
        e1 = base1 + kt * (0.25 * (s - 7.0))
        o1 = baseo + kt * (0.5 * (s - 5.0))
        for m, o in PAIRS:
            if SQUARES[m] != k:
                continue
            a = None
            for axis in range(3):
                v = SPEEDS[m][axis]
                if v == 0:
                    continue
                unit = w[axis]
                if a is None:
                    a = unit if v > 0 else -unit
                else:
                    a = a + unit if v > 0 else a - unit
            if size[k] != 1:
                a = float(size[k]) * a
            q = a * a
            even = e0 + q * (e1 + q * k24)
            odd = a * (o1 + q * k6)
            emit(m, keep * load(m) + (even + odd))
            emit(o, keep * load(o) + (even - odd))


def kernel(
    pop, rate, ext, g, r, zs, zr, y1s, y1r, y2s, y2r,
    in_sem, z_ss, z_rs, y1_ss, y1_rs, y2_ss, y2_rs, x_ss, x_rs,
):
    nx, ny, nz = pop.shape[1:]
    inner = nx - 4
    groups = [(0, 2), (nx - 2, 2), (2, inner)]
    loads = [
        pltpu.make_async_copy(
            pop.at[:, pl.ds(first, count)], g.at[:, pl.ds(first, count)], in_sem.at[n]
        )
        for n, (first, count) in enumerate(groups)
    ]
    loads.append(pltpu.make_async_copy(rate, r, in_sem.at[3]))
    for n in (3, 0, 1, 2):
        loads[n].start()

    around = []
    for axis in AXES:
        n = lax.axis_size(axis)
        me = lax.axis_index(axis)
        around.append(({axis: lax.rem(me + 1, n)}, {axis: lax.rem(me + n - 1, n)}))
    barrier = pltpu.get_barrier_semaphore()
    for pair in around:
        for target in pair:
            pl.semaphore_signal(barrier, inc=1, device_id=target, device_id_type=MESH)

    lane = lax.broadcasted_iota(jnp.int32, (ny, nz), 1)

    def layer_a(j):
        return j + (j // 2) * (nx - 4)

    def layer_b(j):
        return j + 2

    def rows_at(m):
        start = PY + SPEEDS[m][1]
        return pl.ds(start, ny)

    def edge_rows(sign, count):
        return pl.ds(PY + ny, count) if sign == 0 else pl.ds(PY - count, count)

    def home_rows(sign, count):
        return pl.ds(PY, count) if sign == 0 else pl.ds(PY + ny - count, count)

    def collide_chunk(chunk, layer, steps):
        def step(j, packed):
            x = layer(j)
            packed = list(packed)
            mine = [jnp.zeros((ny, nz), jnp.float32), jnp.zeros((ny, nz), jnp.float32)]
            slot = [{m: (s, c) for m, s, c in ZCOLS[d]} for d in (0, 1)]

            def emit(m, value):
                cx, cy, cz = SPEEDS[m]
                if cz:
                    d = 0 if cz > 0 else 1
                    start, count = slot[d][m]
                    shift = start + count if d == 0 else start
                    moved = pltpu.roll(value, shift, 1) if shift else value
                    mask = (lane >= start) & (lane < start + count)
                    mine[d] = jnp.where(mask, moved, mine[d])
                    value = pltpu.roll(value, cz % nz, 1)
                ext[m, PX + x + cx, rows_at(m), :] = value

            collide(lambda m: g[m, x], r[x], emit)
            for d in (0, 1):
                moved = pltpu.roll(mine[d], GROUP * j, 1)
                mask = (lane >= GROUP * j) & (lane < GROUP * j + GROUP)
                packed[d] = jnp.where(mask, moved, packed[d])
            for d in (0, 1):
                for m, start, count in Y1ROWS[d]:
                    y1s[chunk, d, j, pl.ds(start, count), :] = ext[
                        m, PX + x + SPEEDS[m][0], edge_rows(d, count), :
                    ]
            return tuple(packed)

        blank = jnp.zeros((ny, nz), jnp.float32)
        packed = lax.fori_loop(0, steps, step, (blank, blank))
        for d in (0, 1):
            zs[chunk, d] = packed[d]

    def settle_z(chunk, layer, steps):
        def step(j, carry):
            x = layer(j)
            for d in (0, 1):
                back = lax.rem(nz - GROUP * j, nz)
                base = pltpu.roll(zr[chunk, d], back, 1)
                for m, start, count in ZCOLS[d]:
                    shift = start if d == 0 else start + count
                    moved = pltpu.roll(base, nz - shift, 1) if shift else base
                    mask = lane < count if d == 0 else lane >= nz - count
                    where = (m, PX + x + SPEEDS[m][0], rows_at(m), slice(None))
                    ext[where] = jnp.where(mask, moved, ext[where])
            for d in (0, 1):
                for m, start, count in Y2ROWS[d]:
                    y2s[chunk, d, j, pl.ds(start, count), :] = ext[
                        m, PX + x + SPEEDS[m][0], edge_rows(d, count), :
                    ]
            return carry

        lax.fori_loop(0, steps, step, 0)

    def settle_y(chunk, layer, steps, table, received):
        def step(j, carry):
            x = layer(j)
            for d in (0, 1):
                for m, start, count in table[d]:
                    ext[m, PX + x + SPEEDS[m][0], home_rows(d, count), :] = received[
                        chunk, d, j, pl.ds(start, count), :
                    ]
            return carry

        lax.fori_loop(0, steps, step, 0)

    def send_all(axis, chunk, src, dst, ss, rs):
        copies = []
        for d in (0, 1):
            copies.append(
                pltpu.make_async_remote_copy(
                    src_ref=src.at[chunk, d],
                    dst_ref=dst.at[chunk, d],
                    send_sem=ss.at[chunk, d],
                    recv_sem=rs.at[chunk, d],
                    device_id=around[axis][d],
                    device_id_type=MESH,
                )
            )
        for copy in copies:
            copy.start()
        return copies

    xs = []

    def send_x(pair):
        for d in (0, 1):
            first, members, layers = pair[d]
            n = len(xs)
            out_at = PX + nx if d == 0 else PX - layers
            in_at = PX if d == 0 else PX + nx - layers
            which, rows = pl.ds(first, members), pl.ds(PY, ny)
            copy = pltpu.make_async_remote_copy(
                src_ref=ext.at[which, pl.ds(out_at, layers), rows],
                dst_ref=ext.at[which, pl.ds(in_at, layers), rows],
                send_sem=x_ss.at[n],
                recv_sem=x_rs.at[n],
                device_id=around[0][d],
                device_id_type=MESH,
            )
            copy.start()
            xs.append(copy)

    for n in (3, 0, 1):
        loads[n].wait()
    collide_chunk(0, layer_a, 4)
    pl.semaphore_wait(barrier, 6)
    z_a = send_all(2, 0, zs, zr, z_ss, z_rs)
    y1_a = send_all(1, 0, y1s, y1r, y1_ss, y1_rs)
    send_x(XPURE[0])
    send_x(XPURE[1])
    loads[2].wait()
    collide_chunk(1, layer_b, inner)
    z_b = send_all(2, 1, zs, zr, z_ss, z_rs)
    y1_b = send_all(1, 1, y1s, y1r, y1_ss, y1_rs)
    send_x(XPURE[2])

    for copy in z_a:
        copy.wait_recv()
    settle_z(0, layer_a, 4)
    y2_a = send_all(1, 0, y2s, y2r, y2_ss, y2_rs)
    send_x(XZ)
    for copy in y1_a:
        copy.wait_recv()
    settle_y(0, layer_a, 4, Y1ROWS, y1r)
    send_x(XY)
    for copy in z_b:
        copy.wait_recv()
    settle_z(1, layer_b, inner)
    y2_b = send_all(1, 1, y2s, y2r, y2_ss, y2_rs)
    for copy in y2_a:
        copy.wait_recv()
    settle_y(0, layer_a, 4, Y2ROWS, y2r)
    send_x(XYZ)
    for copy in y1_b:
        copy.wait_recv()
    settle_y(1, layer_b, inner, Y1ROWS, y1r)
    for copy in y2_b:
        copy.wait_recv()
    settle_y(1, layer_b, inner, Y2ROWS, y2r)
    for copy in xs:
        copy.wait_recv()
    for copy in z_a + z_b + y1_a + y1_b + y2_a + y2_b + xs:
        copy.wait_send()


def crop(ext, out, sem):
    nx, ny = out.shape[1:3]
    parts = 3
    share = Q // parts
    copies = [
        pltpu.make_async_copy(
            ext.at[pl.ds(n * share, share), pl.ds(PX, nx), pl.ds(PY, ny)],
            out.at[pl.ds(n * share, share)],
            sem.at[n],
        )
        for n in range(parts)
    ]
    for copy in copies:
        copy.start()
    for copy in copies:
        copy.wait()


def per_device(populations, relax):
    nx, ny, nz = relax.shape
    steps = max(4, nx - 4)
    shape = (Q, nx + 2 * PX, ny + 2 * PY, nz)
    f32 = jnp.float32
    dma = pltpu.SemaphoreType.DMA
    any_space = pl.BlockSpec(memory_space=pl.ANY)
    room = 67043328 - 4 * math.prod(shape) - 32768
    ext = pl.pallas_call(
        kernel,
        out_shape=pltpu.VMEM(shape, f32),
        in_specs=[pl.BlockSpec(memory_space=pltpu.HBM)] * 2,
        out_specs=pl.BlockSpec(memory_space=pltpu.VMEM),
        scratch_shapes=[
            pltpu.VMEM((Q, nx, ny, nz), f32),
            pltpu.VMEM((nx, ny, nz), f32),
            pltpu.VMEM((2, 2, ny, nz), f32),
            pltpu.VMEM((2, 2, ny, nz), f32),
            pltpu.VMEM((2, 2, steps, Y1SIZE, nz), f32),
            pltpu.VMEM((2, 2, steps, Y1SIZE, nz), f32),
            pltpu.VMEM((2, 2, steps, Y2SIZE, nz), f32),
            pltpu.VMEM((2, 2, steps, Y2SIZE, nz), f32),
            dma((4,)),
            dma((2, 2)), dma((2, 2)),
            dma((2, 2)), dma((2, 2)),
            dma((2, 2)), dma((2, 2)),
            dma((12,)), dma((12,)),
        ],
        compiler_params=pltpu.CompilerParams(
            collective_id=0, has_side_effects=True, vmem_limit_bytes=room
        ),
    )(populations, relax)
    return pl.pallas_call(
        crop,
        out_shape=jax.ShapeDtypeStruct((Q, nx, ny, nz), f32),
        in_specs=[any_space],
        out_specs=any_space,
        scratch_shapes=[dma((3,))],
        compiler_params=pltpu.CompilerParams(vmem_limit_bytes=2**20),
    )(ext)


def solution(mesh):
    return jax.shard_map(
        per_device,
        mesh=mesh,
        in_specs=(P(None, "gx", "gy", "gz"), P("gx", "gy", "gz")),
        out_specs=P(None, "gx", "gy", "gz"),
        check_vma=False,
    )
```

```python
import math

import jax
import jax.numpy as jnp
from jax import lax
from jax.experimental import pallas as pl
from jax.experimental.pallas import tpu as pltpu
from jax.sharding import PartitionSpec as P

MESH = pl.DeviceIdType.MESH
AXES = ("gx", "gy", "gz")
PX = 3
PY = 8
GROUP = 32


def lattice():
    speeds = [(0, 0, 0)]
    weights = [1.0 / 12.0]
    for axis in range(3):
        for sign in (1, -1):
            vector = [0, 0, 0]
            vector[axis] = sign
            speeds.append(tuple(vector))
            weights.append(1.0 / 12.0)
    for first in (1, -1):
        for second in (1, -1):
            for third in (1, -1):
                speeds.append((first, second, third))
                weights.append(1.0 / 27.0)
    for axis in range(3):
        for sign in (2, -2):
            vector = [0, 0, 0]
            vector[axis] = sign
            speeds.append(tuple(vector))
            weights.append(2.0 / 135.0)
    for couple in ((0, 1), (0, 2), (1, 2)):
        for first in (2, -2):
            for second in (2, -2):
                vector = [0, 0, 0]
                vector[couple[0]] = first
                vector[couple[1]] = second
                speeds.append(tuple(vector))
                weights.append(1.0 / 432.0)
    for axis in range(3):
        for sign in (3, -3):
            vector = [0, 0, 0]
            vector[axis] = sign
            speeds.append(tuple(vector))
            weights.append(1.0 / 1620.0)
    return (speeds, weights)


SPEEDS, WEIGHTS = lattice()
Q = len(SPEEDS)
SQUARES = [sum(v * v for v in c) for c in SPEEDS]
PAIRS = [
    (m, SPEEDS.index(tuple(-v for v in SPEEDS[m])))
    for m in range(1, Q)
    if m < SPEEDS.index(tuple(-v for v in SPEEDS[m]))
]


def offsets(axis, sign, keep):
    rows, start = [], 0
    for m, c in enumerate(SPEEDS):
        count = c[axis] * sign
        if count > 0 and keep(c):
            rows.append((m, start, count))
            start += count
    return rows


ZCOLS = [offsets(2, sign, lambda c: True) for sign in (1, -1)]
Y1ROWS = [offsets(1, sign, lambda c: c[2] == 0) for sign in (1, -1)]
Y2ROWS = [offsets(1, sign, lambda c: c[2] != 0) for sign in (1, -1)]
Y1SIZE, Y2SIZE = 16, 8

XPURE = [[(SPEEDS.index((s * k, 0, 0)), 1, k) for s in (1, -1)] for k in (1, 2, 3)]
XZ = [(SPEEDS.index((s * 2, 0, 2)), 2, 2) for s in (1, -1)]
XY = [[(SPEEDS.index((s * 2, k, 0)), 1, 2) for s in (1, -1)] for k in (2, -2)]
XYZ = [[(SPEEDS.index((s, k, 1)), 2, 1) for s in (1, -1)] for k in (1, -1)]


def add_all(terms):
    total = terms[0]
    for term in terms[1:]:
        total = total + term
    return total


def collide(load, rate, emit):
    sums = {k: [] for k in (1, 3, 4, 8, 9)}
    flows = {k: [[], [], []] for k in (1, 3, 4, 8, 9)}
    for m, o in PAIRS:
        up, down = load(m), load(o)
        k = SQUARES[m]
        sums[k].append(up + down)
        diff = up - down
        for axis in range(3):
            if SPEEDS[m][axis] > 0:
                flows[k][axis].append((1, diff))
            elif SPEEDS[m][axis] < 0:
                flows[k][axis].append((-1, diff))
    weight = {SQUARES[m]: WEIGHTS[m] for m in range(Q)}
    size = {1: 1, 3: 1, 4: 2, 8: 2, 9: 3}
    rest = load(0)
    groups = {k: add_all(sums[k]) for k in sums}
    rho = weight[0] * rest
    energy = None
    for k in sums:
        part = weight[k] * groups[k]
        rho = rho + part
        part = part if k == 1 else float(k) * part
        energy = part if energy is None else energy + part
    flux = []
    for axis in range(3):
        total = None
        for k in flows:
            part = None
            for sign, diff in flows[k][axis]:
                if part is None:
                    part = diff if sign > 0 else -diff
                else:
                    part = part + diff if sign > 0 else part - diff
            part = (weight[k] * size[k]) * part
            total = part if total is None else total + part
        flux.append(total)
    inverse = 1.0 / rho
    velocity = [part * inverse for part in flux]
    norm = velocity[0] * velocity[0] + velocity[1] * velocity[1] + velocity[2] * velocity[2]
    t = (energy * inverse - norm) * 0.5 - 1.0
    b = 1.5 * norm
    w = [1.5 * part for part in velocity]
    keep = 1.0 - rate
    k0 = rho * rate
    k24 = k0 * (1.0 / 24.0)
    k6 = k0 * (1.0 / 6.0)
    half_b = 0.5 * b
    kt = k0 * t
    ktb = kt * b
    ktt = kt * t
    base = k0 * (1.0 - half_b + 0.5 * half_b * half_b)
    base1 = k0 * (0.5 - 0.5 * half_b)
    baseo = k0 * (1.0 - half_b)

    def even0(s):
        return (
            base
            + kt * (0.5 * (s - 3.0))
            + ktb * (0.25 * (5.0 - s))
            + ktt * ((s * s - 10.0 * s + 15.0) / 8.0)
        )

    emit(0, keep * rest + even0(0.0))
    for k in sums:
        s = 1.5 * k
        e0 = even0(s)
        e1 = base1 + kt * (0.25 * (s - 7.0))
        o1 = baseo + kt * (0.5 * (s - 5.0))
        for m, o in PAIRS:
            if SQUARES[m] != k:
                continue
            a = None
            for axis in range(3):
                v = SPEEDS[m][axis]
                if v == 0:
                    continue
                unit = w[axis]
                if a is None:
                    a = unit if v > 0 else -unit
                else:
                    a = a + unit if v > 0 else a - unit
            if size[k] != 1:
                a = float(size[k]) * a
            q = a * a
            even = e0 + q * (e1 + q * k24)
            odd = a * (o1 + q * k6)
            emit(m, keep * load(m) + (even + odd))
            emit(o, keep * load(o) + (even - odd))


def kernel(
    pop, rate, ext, g, r, zs, zr, y1s, y1r, y2s, y2r,
    in_sem, z_ss, z_rs, y1_ss, y1_rs, y2_ss, y2_rs, x_ss, x_rs,
):
    nx, ny, nz = pop.shape[1:]
    inner = nx - 4
    groups = [(0, 2), (nx - 2, 2), (2, inner)]
    loads = [
        pltpu.make_async_copy(
            pop.at[:, pl.ds(first, count)], g.at[:, pl.ds(first, count)], in_sem.at[n]
        )
        for n, (first, count) in enumerate(groups)
    ]
    loads.append(pltpu.make_async_copy(rate, r, in_sem.at[3]))
    for n in (3, 0, 1, 2):
        loads[n].start()

    around = []
    for axis in AXES:
        n = lax.axis_size(axis)
        me = lax.axis_index(axis)
        around.append(({axis: lax.rem(me + 1, n)}, {axis: lax.rem(me + n - 1, n)}))
    barrier = pltpu.get_barrier_semaphore()
    for pair in around:
        for target in pair:
            pl.semaphore_signal(barrier, inc=1, device_id=target, device_id_type=MESH)

    lane = lax.broadcasted_iota(jnp.int32, (ny, nz), 1)

    def layer_a(j):
        return j + (j // 2) * (nx - 4)

    def layer_b(j):
        return j + 2

    def rows_at(m):
        start = PY + SPEEDS[m][1]
        return pl.ds(start, ny)

    def edge_rows(sign, count):
        return pl.ds(PY + ny, count) if sign == 0 else pl.ds(PY - count, count)

    def home_rows(sign, count):
        return pl.ds(PY, count) if sign == 0 else pl.ds(PY + ny - count, count)

    def collide_chunk(chunk, layer, steps):
        def step(j, packed):
            x = layer(j)
            packed = list(packed)
            mine = [jnp.zeros((ny, nz), jnp.float32), jnp.zeros((ny, nz), jnp.float32)]
            slot = [{m: (s, c) for m, s, c in ZCOLS[d]} for d in (0, 1)]

            def emit(m, value):
                cx, cy, cz = SPEEDS[m]
                if cz:
                    d = 0 if cz > 0 else 1
                    start, count = slot[d][m]
                    shift = start + count if d == 0 else start
                    moved = pltpu.roll(value, shift, 1) if shift else value
                    mask = (lane >= start) & (lane < start + count)
                    mine[d] = jnp.where(mask, moved, mine[d])
                    value = pltpu.roll(value, cz % nz, 1)
                ext[m, PX + x + cx, rows_at(m), :] = value

            collide(lambda m: g[m, x], r[x], emit)
            for d in (0, 1):
                moved = pltpu.roll(mine[d], GROUP * j, 1)
                mask = (lane >= GROUP * j) & (lane < GROUP * j + GROUP)
                packed[d] = jnp.where(mask, moved, packed[d])
            for d in (0, 1):
                for m, start, count in Y1ROWS[d]:
                    y1s[chunk, d, j, pl.ds(start, count), :] = ext[
                        m, PX + x + SPEEDS[m][0], edge_rows(d, count), :
                    ]
            return tuple(packed)

        blank = jnp.zeros((ny, nz), jnp.float32)
        packed = lax.fori_loop(0, steps, step, (blank, blank))
        for d in (0, 1):
            zs[chunk, d] = packed[d]

    def settle_z(chunk, layer, steps):
        def step(j, carry):
            x = layer(j)
            for d in (0, 1):
                back = lax.rem(nz - GROUP * j, nz)
                base = pltpu.roll(zr[chunk, d], back, 1)
                for m, start, count in ZCOLS[d]:
                    shift = start if d == 0 else start + count
                    moved = pltpu.roll(base, nz - shift, 1) if shift else base
                    mask = lane < count if d == 0 else lane >= nz - count
                    where = (m, PX + x + SPEEDS[m][0], rows_at(m), slice(None))
                    ext[where] = jnp.where(mask, moved, ext[where])
            for d in (0, 1):
                for m, start, count in Y2ROWS[d]:
                    y2s[chunk, d, j, pl.ds(start, count), :] = ext[
                        m, PX + x + SPEEDS[m][0], edge_rows(d, count), :
                    ]
            return carry

        lax.fori_loop(0, steps, step, 0)

    def settle_y(chunk, layer, steps, table, received):
        def step(j, carry):
            x = layer(j)
            for d in (0, 1):
                for m, start, count in table[d]:
                    ext[m, PX + x + SPEEDS[m][0], home_rows(d, count), :] = received[
                        chunk, d, j, pl.ds(start, count), :
                    ]
            return carry

        lax.fori_loop(0, steps, step, 0)

    def send_all(axis, chunk, src, dst, ss, rs):
        copies = []
        for d in (0, 1):
            copies.append(
                pltpu.make_async_remote_copy(
                    src_ref=src.at[chunk, d],
                    dst_ref=dst.at[chunk, d],
                    send_sem=ss.at[chunk, d],
                    recv_sem=rs.at[chunk, d],
                    device_id=around[axis][d],
                    device_id_type=MESH,
                )
            )
        for copy in copies:
            copy.start()
        return copies

    xs = []
    early = [(8, ny - 8), (0, ny - 8)]
    late = [(0, 8), (ny - 8, 8)]

    def send_x(pair, rows=None):
        start, count = rows or (0, ny)
        for d in (0, 1):
            first, members, layers = pair[d]
            n = len(xs)
            out_at = PX + nx if d == 0 else PX - layers
            in_at = PX if d == 0 else PX + nx - layers
            which, rows = pl.ds(first, members), pl.ds(PY + start, count)
            copy = pltpu.make_async_remote_copy(
                src_ref=ext.at[which, pl.ds(out_at, layers), rows],
                dst_ref=ext.at[which, pl.ds(in_at, layers), rows],
                send_sem=x_ss.at[n],
                recv_sem=x_rs.at[n],
                device_id=around[0][d],
                device_id_type=MESH,
            )
            copy.start()
            xs.append(copy)

    for n in (3, 0, 1):
        loads[n].wait()
    collide_chunk(0, layer_a, 4)
    pl.semaphore_wait(barrier, 6)
    z_a = send_all(2, 0, zs, zr, z_ss, z_rs)
    y1_a = send_all(1, 0, y1s, y1r, y1_ss, y1_rs)
    send_x(XPURE[0])
    send_x(XPURE[1])
    for n in (0, 1):
        send_x(XY[n], early[n])
    loads[2].wait()
    collide_chunk(1, layer_b, inner)
    z_b = send_all(2, 1, zs, zr, z_ss, z_rs)
    y1_b = send_all(1, 1, y1s, y1r, y1_ss, y1_rs)
    send_x(XPURE[2])

    for copy in z_a:
        copy.wait_recv()
    settle_z(0, layer_a, 4)
    y2_a = send_all(1, 0, y2s, y2r, y2_ss, y2_rs)
    send_x(XZ)
    for n in (0, 1):
        send_x(XYZ[n], early[n])
    for copy in y1_a:
        copy.wait_recv()
    settle_y(0, layer_a, 4, Y1ROWS, y1r)
    for n in (0, 1):
        send_x(XY[n], late[n])
    for copy in z_b:
        copy.wait_recv()
    settle_z(1, layer_b, inner)
    y2_b = send_all(1, 1, y2s, y2r, y2_ss, y2_rs)
    for copy in y2_a:
        copy.wait_recv()
    settle_y(0, layer_a, 4, Y2ROWS, y2r)
    for n in (0, 1):
        send_x(XYZ[n], late[n])
    for copy in y1_b:
        copy.wait_recv()
    settle_y(1, layer_b, inner, Y1ROWS, y1r)
    for copy in y2_b:
        copy.wait_recv()
    settle_y(1, layer_b, inner, Y2ROWS, y2r)
    for copy in xs:
        copy.wait_recv()
    for copy in z_a + z_b + y1_a + y1_b + y2_a + y2_b + xs:
        copy.wait_send()


def crop(ext, out, sem):
    nx, ny = out.shape[1:3]
    parts = 3
    share = Q // parts
    copies = [
        pltpu.make_async_copy(
            ext.at[pl.ds(n * share, share), pl.ds(PX, nx), pl.ds(PY, ny)],
            out.at[pl.ds(n * share, share)],
            sem.at[n],
        )
        for n in range(parts)
    ]
    for copy in copies:
        copy.start()
    for copy in copies:
        copy.wait()


def per_device(populations, relax):
    nx, ny, nz = relax.shape
    steps = max(4, nx - 4)
    shape = (Q, nx + 2 * PX, ny + 2 * PY, nz)
    f32 = jnp.float32
    dma = pltpu.SemaphoreType.DMA
    any_space = pl.BlockSpec(memory_space=pl.ANY)
    room = 67043328 - 4 * math.prod(shape) - 32768
    ext = pl.pallas_call(
        kernel,
        out_shape=pltpu.VMEM(shape, f32),
        in_specs=[pl.BlockSpec(memory_space=pltpu.HBM)] * 2,
        out_specs=pl.BlockSpec(memory_space=pltpu.VMEM),
        scratch_shapes=[
            pltpu.VMEM((Q, nx, ny, nz), f32),
            pltpu.VMEM((nx, ny, nz), f32),
            pltpu.VMEM((2, 2, ny, nz), f32),
            pltpu.VMEM((2, 2, ny, nz), f32),
            pltpu.VMEM((2, 2, steps, Y1SIZE, nz), f32),
            pltpu.VMEM((2, 2, steps, Y1SIZE, nz), f32),
            pltpu.VMEM((2, 2, steps, Y2SIZE, nz), f32),
            pltpu.VMEM((2, 2, steps, Y2SIZE, nz), f32),
            dma((4,)),
            dma((2, 2)), dma((2, 2)),
            dma((2, 2)), dma((2, 2)),
            dma((2, 2)), dma((2, 2)),
            dma((24,)), dma((24,)),
        ],
        compiler_params=pltpu.CompilerParams(
            collective_id=0, has_side_effects=True, vmem_limit_bytes=room
        ),
    )(populations, relax)
    return pl.pallas_call(
        crop,
        out_shape=jax.ShapeDtypeStruct((Q, nx, ny, nz), f32),
        in_specs=[any_space],
        out_specs=any_space,
        scratch_shapes=[dma((3,))],
        compiler_params=pltpu.CompilerParams(vmem_limit_bytes=2**20),
    )(ext)


def solution(mesh):
    return jax.shard_map(
        per_device,
        mesh=mesh,
        in_specs=(P(None, "gx", "gy", "gz"), P("gx", "gy", "gz")),
        out_specs=P(None, "gx", "gy", "gz"),
        check_vma=False,
    )
```

```python
import math

import jax
import jax.numpy as jnp
from jax import lax
from jax.experimental import pallas as pl
from jax.experimental.pallas import tpu as pltpu
from jax.sharding import PartitionSpec as P

MESH = pl.DeviceIdType.MESH
AXES = ("gx", "gy", "gz")
PX = 3
PY = 8
GROUP = 32


def lattice():
    speeds = [(0, 0, 0)]
    weights = [1.0 / 12.0]
    for axis in range(3):
        for sign in (1, -1):
            vector = [0, 0, 0]
            vector[axis] = sign
            speeds.append(tuple(vector))
            weights.append(1.0 / 12.0)
    for first in (1, -1):
        for second in (1, -1):
            for third in (1, -1):
                speeds.append((first, second, third))
                weights.append(1.0 / 27.0)
    for axis in range(3):
        for sign in (2, -2):
            vector = [0, 0, 0]
            vector[axis] = sign
            speeds.append(tuple(vector))
            weights.append(2.0 / 135.0)
    for couple in ((0, 1), (0, 2), (1, 2)):
        for first in (2, -2):
            for second in (2, -2):
                vector = [0, 0, 0]
                vector[couple[0]] = first
                vector[couple[1]] = second
                speeds.append(tuple(vector))
                weights.append(1.0 / 432.0)
    for axis in range(3):
        for sign in (3, -3):
            vector = [0, 0, 0]
            vector[axis] = sign
            speeds.append(tuple(vector))
            weights.append(1.0 / 1620.0)
    return (speeds, weights)


SPEEDS, WEIGHTS = lattice()
Q = len(SPEEDS)
SQUARES = [sum(v * v for v in c) for c in SPEEDS]
PAIRS = [
    (m, SPEEDS.index(tuple(-v for v in SPEEDS[m])))
    for m in range(1, Q)
    if m < SPEEDS.index(tuple(-v for v in SPEEDS[m]))
]


def offsets(axis, sign, keep):
    rows, start = [], 0
    for m, c in enumerate(SPEEDS):
        count = c[axis] * sign
        if count > 0 and keep(c):
            rows.append((m, start, count))
            start += count
    return rows


ZCOLS = [offsets(2, sign, lambda c: True) for sign in (1, -1)]
Y1ROWS = [offsets(1, sign, lambda c: c[2] == 0) for sign in (1, -1)]
Y2ROWS = [offsets(1, sign, lambda c: c[2] != 0) for sign in (1, -1)]
Y1SIZE, Y2SIZE = 16, 8

XPURE = [[(SPEEDS.index((s * k, 0, 0)), 1, k) for s in (1, -1)] for k in (1, 2, 3)]
XZ = [(SPEEDS.index((s * 2, 0, 2)), 2, 2) for s in (1, -1)]
XY = [[(SPEEDS.index((s * 2, k, 0)), 1, 2) for s in (1, -1)] for k in (2, -2)]
XYZ = [[(SPEEDS.index((s, k, 1)), 2, 1) for s in (1, -1)] for k in (1, -1)]


def add_all(terms):
    total = terms[0]
    for term in terms[1:]:
        total = total + term
    return total


def collide(load, rate, emit):
    sums = {k: [] for k in (1, 3, 4, 8, 9)}
    flows = {k: [[], [], []] for k in (1, 3, 4, 8, 9)}
    for m, o in PAIRS:
        up, down = load(m), load(o)
        k = SQUARES[m]
        sums[k].append(up + down)
        diff = up - down
        for axis in range(3):
            if SPEEDS[m][axis] > 0:
                flows[k][axis].append((1, diff))
            elif SPEEDS[m][axis] < 0:
                flows[k][axis].append((-1, diff))
    weight = {SQUARES[m]: WEIGHTS[m] for m in range(Q)}
    size = {1: 1, 3: 1, 4: 2, 8: 2, 9: 3}
    rest = load(0)
    groups = {k: add_all(sums[k]) for k in sums}
    rho = weight[0] * rest
    energy = None
    for k in sums:
        part = weight[k] * groups[k]
        rho = rho + part
        part = part if k == 1 else float(k) * part
        energy = part if energy is None else energy + part
    flux = []
    for axis in range(3):
        total = None
        for k in flows:
            part = None
            for sign, diff in flows[k][axis]:
                if part is None:
                    part = diff if sign > 0 else -diff
                else:
                    part = part + diff if sign > 0 else part - diff
            part = (weight[k] * size[k]) * part
            total = part if total is None else total + part
        flux.append(total)
    inverse = 1.0 / rho
    velocity = [part * inverse for part in flux]
    norm = velocity[0] * velocity[0] + velocity[1] * velocity[1] + velocity[2] * velocity[2]
    t = (energy * inverse - norm) * 0.5 - 1.0
    b = 1.5 * norm
    w = [1.5 * part for part in velocity]
    keep = 1.0 - rate
    k0 = rho * rate
    k24 = k0 * (1.0 / 24.0)
    k6 = k0 * (1.0 / 6.0)
    half_b = 0.5 * b
    kt = k0 * t
    ktb = kt * b
    ktt = kt * t
    base = k0 * (1.0 - half_b + 0.5 * half_b * half_b)
    base1 = k0 * (0.5 - 0.5 * half_b)
    baseo = k0 * (1.0 - half_b)

    def even0(s):
        return (
            base
            + kt * (0.5 * (s - 3.0))
            + ktb * (0.25 * (5.0 - s))
            + ktt * ((s * s - 10.0 * s + 15.0) / 8.0)
        )

    emit(0, keep * rest + even0(0.0))
    for k in sums:
        s = 1.5 * k
        e0 = even0(s)
        e1 = base1 + kt * (0.25 * (s - 7.0))
        o1 = baseo + kt * (0.5 * (s - 5.0))
        for m, o in PAIRS:
            if SQUARES[m] != k:
                continue
            a = None
            for axis in range(3):
                v = SPEEDS[m][axis]
                if v == 0:
                    continue
                unit = w[axis]
                if a is None:
                    a = unit if v > 0 else -unit
                else:
                    a = a + unit if v > 0 else a - unit
            if size[k] != 1:
                a = float(size[k]) * a
            q = a * a
            even = e0 + q * (e1 + q * k24)
            odd = a * (o1 + q * k6)
            emit(m, keep * load(m) + (even + odd))
            emit(o, keep * load(o) + (even - odd))


def kernel(
    pop, rate, ext, g, r, zs, zr, y1s, y1r, y2s, y2r,
    in_sem, z_ss, z_rs, y1_ss, y1_rs, y2_ss, y2_rs, x_ss, x_rs, token,
):
    nx, ny, nz = pop.shape[1:]
    inner = nx - 4
    groups = [(0, 2), (nx - 2, 2), (2, inner)]
    loads = [
        pltpu.make_async_copy(
            pop.at[:, pl.ds(first, count)], g.at[:, pl.ds(first, count)], in_sem.at[n]
        )
        for n, (first, count) in enumerate(groups)
    ]
    loads.append(pltpu.make_async_copy(rate, r, in_sem.at[3]))
    for n in (3, 0, 1, 2):
        loads[n].start()

    around = []
    for axis in AXES:
        n = lax.axis_size(axis)
        me = lax.axis_index(axis)
        around.append(({axis: lax.rem(me + 1, n)}, {axis: lax.rem(me + n - 1, n)}))
    barrier = pltpu.get_barrier_semaphore()
    for axis in (0, 2):
        for target in around[axis]:
            pl.semaphore_signal(barrier, inc=1, device_id=target, device_id_type=MESH)
    long = lax.axis_size("gy")
    row = lax.axis_index("gy")
    relayed = long > 2
    ends = (long - 1, 0)
    for d in (0, 1):
        if relayed:
            @pl.when(row != ends[d])
            def _():
                pl.semaphore_signal(barrier, inc=1, device_id=around[1][d], device_id_type=MESH)
        else:
            pl.semaphore_signal(barrier, inc=1, device_id=around[1][d], device_id_type=MESH)

    def relay(d):
        @pl.when(row != ends[1 - d])
        def _():
            pl.semaphore_wait(token.at[d], 1)

        @pl.when(row != ends[d])
        def _():
            pl.semaphore_signal(token.at[d], inc=1, device_id=around[1][d], device_id_type=MESH)

    def relay_near(first):
        if not relayed:
            return

        @pl.when(row < long // 2 if first else row >= long // 2)
        def _():
            relay(0)

        @pl.when(row >= long // 2 if first else row < long // 2)
        def _():
            relay(1)

    lane = lax.broadcasted_iota(jnp.int32, (ny, nz), 1)

    def layer_a(j):
        return j + (j // 2) * (nx - 4)

    def layer_b(j):
        return j + 2

    def rows_at(m):
        start = PY + SPEEDS[m][1]
        return pl.ds(start, ny)

    def edge_rows(sign, count):
        return pl.ds(PY + ny, count) if sign == 0 else pl.ds(PY - count, count)

    def home_rows(sign, count):
        return pl.ds(PY, count) if sign == 0 else pl.ds(PY + ny - count, count)

    def collide_chunk(chunk, layer, steps):
        def step(j, packed):
            x = layer(j)
            packed = list(packed)
            mine = [jnp.zeros((ny, nz), jnp.float32), jnp.zeros((ny, nz), jnp.float32)]
            slot = [{m: (s, c) for m, s, c in ZCOLS[d]} for d in (0, 1)]

            def emit(m, value):
                cx, cy, cz = SPEEDS[m]
                if cz:
                    d = 0 if cz > 0 else 1
                    start, count = slot[d][m]
                    shift = start + count if d == 0 else start
                    moved = pltpu.roll(value, shift, 1) if shift else value
                    mask = (lane >= start) & (lane < start + count)
                    mine[d] = jnp.where(mask, moved, mine[d])
                    value = pltpu.roll(value, cz % nz, 1)
                ext[m, PX + x + cx, rows_at(m), :] = value

            collide(lambda m: g[m, x], r[x], emit)
            for d in (0, 1):
                moved = pltpu.roll(mine[d], GROUP * j, 1)
                mask = (lane >= GROUP * j) & (lane < GROUP * j + GROUP)
                packed[d] = jnp.where(mask, moved, packed[d])
            for d in (0, 1):
                for m, start, count in Y1ROWS[d]:
                    y1s[chunk, d, j, pl.ds(start, count), :] = ext[
                        m, PX + x + SPEEDS[m][0], edge_rows(d, count), :
                    ]
            return tuple(packed)

        blank = jnp.zeros((ny, nz), jnp.float32)
        packed = lax.fori_loop(0, steps, step, (blank, blank))
        for d in (0, 1):
            zs[chunk, d] = packed[d]

    def settle_z(chunk, layer, steps):
        def step(j, carry):
            x = layer(j)
            for d in (0, 1):
                back = lax.rem(nz - GROUP * j, nz)
                base = pltpu.roll(zr[chunk, d], back, 1)
                for m, start, count in ZCOLS[d]:
                    shift = start if d == 0 else start + count
                    moved = pltpu.roll(base, nz - shift, 1) if shift else base
                    mask = lane < count if d == 0 else lane >= nz - count
                    where = (m, PX + x + SPEEDS[m][0], rows_at(m), slice(None))
                    ext[where] = jnp.where(mask, moved, ext[where])
            for d in (0, 1):
                for m, start, count in Y2ROWS[d]:
                    y2s[chunk, d, j, pl.ds(start, count), :] = ext[
                        m, PX + x + SPEEDS[m][0], edge_rows(d, count), :
                    ]
            return carry

        lax.fori_loop(0, steps, step, 0)

    def settle_y(chunk, layer, steps, table, received):
        def step(j, carry):
            x = layer(j)
            for d in (0, 1):
                for m, start, count in table[d]:
                    ext[m, PX + x + SPEEDS[m][0], home_rows(d, count), :] = received[
                        chunk, d, j, pl.ds(start, count), :
                    ]
            return carry

        lax.fori_loop(0, steps, step, 0)

    def send_all(axis, chunk, src, dst, ss, rs, start=True):
        copies = []
        for d in (0, 1):
            copies.append(
                pltpu.make_async_remote_copy(
                    src_ref=src.at[chunk, d],
                    dst_ref=dst.at[chunk, d],
                    send_sem=ss.at[chunk, d],
                    recv_sem=rs.at[chunk, d],
                    device_id=around[axis][d],
                    device_id_type=MESH,
                )
            )
        if start:
            for copy in copies:
                copy.start()
        return copies

    def start_y(copies, wrap):
        for d in (0, 1):
            if not relayed:
                if not wrap:
                    copies[d].start()
                continue

            @pl.when(row == ends[d] if wrap else row != ends[d])
            def _():
                copies[d].start()

    xs = []
    early = [(8, ny - 8), (0, ny - 8)]
    late = [(0, 8), (ny - 8, 8)]

    def send_x(pair, rows=None):
        start, count = rows or (0, ny)
        for d in (0, 1):
            first, members, layers = pair[d]
            n = len(xs)
            out_at = PX + nx if d == 0 else PX - layers
            in_at = PX if d == 0 else PX + nx - layers
            which, rows = pl.ds(first, members), pl.ds(PY + start, count)
            copy = pltpu.make_async_remote_copy(
                src_ref=ext.at[which, pl.ds(out_at, layers), rows],
                dst_ref=ext.at[which, pl.ds(in_at, layers), rows],
                send_sem=x_ss.at[n],
                recv_sem=x_rs.at[n],
                device_id=around[0][d],
                device_id_type=MESH,
            )
            copy.start()
            xs.append(copy)

    for n in (3, 0, 1):
        loads[n].wait()
    collide_chunk(0, layer_a, 4)
    if relayed:
        at_end = (row == 0) | (row == long - 1)

        @pl.when(at_end)
        def _():
            pl.semaphore_wait(barrier, 5)

        @pl.when(jnp.logical_not(at_end))
        def _():
            pl.semaphore_wait(barrier, 6)
    else:
        pl.semaphore_wait(barrier, 6)
    z_a = send_all(2, 0, zs, zr, z_ss, z_rs)
    y1_a = send_all(1, 0, y1s, y1r, y1_ss, y1_rs, start=False)
    start_y(y1_a, False)
    send_x(XPURE[0])
    send_x(XPURE[1])
    for n in (0, 1):
        send_x(XY[n], early[n])
    loads[2].wait()
    relay_near(True)
    collide_chunk(1, layer_b, inner)
    relay_near(False)
    start_y(y1_a, True)
    z_b = send_all(2, 1, zs, zr, z_ss, z_rs)
    y1_b = send_all(1, 1, y1s, y1r, y1_ss, y1_rs)
    send_x(XPURE[2])

    for copy in z_a:
        copy.wait_recv()
    settle_z(0, layer_a, 4)
    y2_a = send_all(1, 0, y2s, y2r, y2_ss, y2_rs)
    send_x(XZ)
    for n in (0, 1):
        send_x(XYZ[n], early[n])
    for copy in y1_a:
        copy.wait_recv()
    settle_y(0, layer_a, 4, Y1ROWS, y1r)
    for n in (0, 1):
        send_x(XY[n], late[n])
    for copy in z_b:
        copy.wait_recv()
    settle_z(1, layer_b, inner)
    y2_b = send_all(1, 1, y2s, y2r, y2_ss, y2_rs)
    for copy in y2_a:
        copy.wait_recv()
    settle_y(0, layer_a, 4, Y2ROWS, y2r)
    for n in (0, 1):
        send_x(XYZ[n], late[n])
    for copy in y1_b:
        copy.wait_recv()
    settle_y(1, layer_b, inner, Y1ROWS, y1r)
    for copy in y2_b:
        copy.wait_recv()
    settle_y(1, layer_b, inner, Y2ROWS, y2r)
    for copy in xs:
        copy.wait_recv()
    for copy in z_a + z_b + y1_a + y1_b + y2_a + y2_b + xs:
        copy.wait_send()


def crop(ext, out, sem):
    nx, ny = out.shape[1:3]
    parts = 3
    share = Q // parts
    copies = [
        pltpu.make_async_copy(
            ext.at[pl.ds(n * share, share), pl.ds(PX, nx), pl.ds(PY, ny)],
            out.at[pl.ds(n * share, share)],
            sem.at[n],
        )
        for n in range(parts)
    ]
    for copy in copies:
        copy.start()
    for copy in copies:
        copy.wait()


def per_device(populations, relax):
    nx, ny, nz = relax.shape
    steps = max(4, nx - 4)
    shape = (Q, nx + 2 * PX, ny + 2 * PY, nz)
    f32 = jnp.float32
    dma = pltpu.SemaphoreType.DMA
    any_space = pl.BlockSpec(memory_space=pl.ANY)
    room = 67043328 - 4 * math.prod(shape) - 32768
    ext = pl.pallas_call(
        kernel,
        out_shape=pltpu.VMEM(shape, f32),
        in_specs=[pl.BlockSpec(memory_space=pltpu.HBM)] * 2,
        out_specs=pl.BlockSpec(memory_space=pltpu.VMEM),
        scratch_shapes=[
            pltpu.VMEM((Q, nx, ny, nz), f32),
            pltpu.VMEM((nx, ny, nz), f32),
            pltpu.VMEM((2, 2, ny, nz), f32),
            pltpu.VMEM((2, 2, ny, nz), f32),
            pltpu.VMEM((2, 2, steps, Y1SIZE, nz), f32),
            pltpu.VMEM((2, 2, steps, Y1SIZE, nz), f32),
            pltpu.VMEM((2, 2, steps, Y2SIZE, nz), f32),
            pltpu.VMEM((2, 2, steps, Y2SIZE, nz), f32),
            dma((4,)),
            dma((2, 2)), dma((2, 2)),
            dma((2, 2)), dma((2, 2)),
            dma((2, 2)), dma((2, 2)),
            dma((24,)), dma((24,)),
            pltpu.SemaphoreType.REGULAR((2,)),
        ],
        compiler_params=pltpu.CompilerParams(
            collective_id=0, has_side_effects=True, vmem_limit_bytes=room
        ),
    )(populations, relax)
    return pl.pallas_call(
        crop,
        out_shape=jax.ShapeDtypeStruct((Q, nx, ny, nz), f32),
        in_specs=[any_space],
        out_specs=any_space,
        scratch_shapes=[dma((3,))],
        compiler_params=pltpu.CompilerParams(vmem_limit_bytes=2**20),
    )(ext)


def solution(mesh):
    return jax.shard_map(
        per_device,
        mesh=mesh,
        in_specs=(P(None, "gx", "gy", "gz"), P("gx", "gy", "gz")),
        out_specs=P(None, "gx", "gy", "gz"),
        check_vma=False,
    )
```

```python
import math

import jax
import jax.numpy as jnp
from jax import lax
from jax.experimental import pallas as pl
from jax.experimental.pallas import tpu as pltpu
from jax.sharding import PartitionSpec as P

MESH = pl.DeviceIdType.MESH
AXES = ("gx", "gy", "gz")
PX = 3
PY = 8
GROUP = 32


def lattice():
    speeds = [(0, 0, 0)]
    weights = [1.0 / 12.0]
    for axis in range(3):
        for sign in (1, -1):
            vector = [0, 0, 0]
            vector[axis] = sign
            speeds.append(tuple(vector))
            weights.append(1.0 / 12.0)
    for first in (1, -1):
        for second in (1, -1):
            for third in (1, -1):
                speeds.append((first, second, third))
                weights.append(1.0 / 27.0)
    for axis in range(3):
        for sign in (2, -2):
            vector = [0, 0, 0]
            vector[axis] = sign
            speeds.append(tuple(vector))
            weights.append(2.0 / 135.0)
    for couple in ((0, 1), (0, 2), (1, 2)):
        for first in (2, -2):
            for second in (2, -2):
                vector = [0, 0, 0]
                vector[couple[0]] = first
                vector[couple[1]] = second
                speeds.append(tuple(vector))
                weights.append(1.0 / 432.0)
    for axis in range(3):
        for sign in (3, -3):
            vector = [0, 0, 0]
            vector[axis] = sign
            speeds.append(tuple(vector))
            weights.append(1.0 / 1620.0)
    return (speeds, weights)


SPEEDS, WEIGHTS = lattice()
Q = len(SPEEDS)
SQUARES = [sum(v * v for v in c) for c in SPEEDS]
PAIRS = [
    (m, SPEEDS.index(tuple(-v for v in SPEEDS[m])))
    for m in range(1, Q)
    if m < SPEEDS.index(tuple(-v for v in SPEEDS[m]))
]


def offsets(axis, sign, keep):
    rows, start = [], 0
    for m, c in enumerate(SPEEDS):
        count = c[axis] * sign
        if count > 0 and keep(c):
            rows.append((m, start, count))
            start += count
    return rows


ZCOLS = [offsets(2, sign, lambda c: True) for sign in (1, -1)]
Y1ROWS = [offsets(1, sign, lambda c: c[2] == 0) for sign in (1, -1)]
Y2ROWS = [offsets(1, sign, lambda c: c[2] != 0) for sign in (1, -1)]
Y1SIZE, Y2SIZE = 16, 8

XPURE = [[(SPEEDS.index((s * k, 0, 0)), 1, k) for s in (1, -1)] for k in (1, 2, 3)]
XZ = [(SPEEDS.index((s * 2, 0, 2)), 2, 2) for s in (1, -1)]
XY = [[(SPEEDS.index((s * 2, k, 0)), 1, 2) for s in (1, -1)] for k in (2, -2)]
XYZ = [[(SPEEDS.index((s, k, 1)), 2, 1) for s in (1, -1)] for k in (1, -1)]


def add_all(terms):
    total = terms[0]
    for term in terms[1:]:
        total = total + term
    return total


def collide(load, rate, emit):
    sums = {k: [] for k in (1, 3, 4, 8, 9)}
    flows = {k: [[], [], []] for k in (1, 3, 4, 8, 9)}
    for m, o in PAIRS:
        up, down = load(m), load(o)
        k = SQUARES[m]
        sums[k].append(up + down)
        diff = up - down
        for axis in range(3):
            if SPEEDS[m][axis] > 0:
                flows[k][axis].append((1, diff))
            elif SPEEDS[m][axis] < 0:
                flows[k][axis].append((-1, diff))
    weight = {SQUARES[m]: WEIGHTS[m] for m in range(Q)}
    size = {1: 1, 3: 1, 4: 2, 8: 2, 9: 3}
    rest = load(0)
    groups = {k: add_all(sums[k]) for k in sums}
    rho = weight[0] * rest
    energy = None
    for k in sums:
        part = weight[k] * groups[k]
        rho = rho + part
        part = part if k == 1 else float(k) * part
        energy = part if energy is None else energy + part
    flux = []
    for axis in range(3):
        total = None
        for k in flows:
            part = None
            for sign, diff in flows[k][axis]:
                if part is None:
                    part = diff if sign > 0 else -diff
                else:
                    part = part + diff if sign > 0 else part - diff
            part = (weight[k] * size[k]) * part
            total = part if total is None else total + part
        flux.append(total)
    inverse = 1.0 / rho
    velocity = [part * inverse for part in flux]
    norm = velocity[0] * velocity[0] + velocity[1] * velocity[1] + velocity[2] * velocity[2]
    t = (energy * inverse - norm) * 0.5 - 1.0
    b = 1.5 * norm
    w = [1.5 * part for part in velocity]
    keep = 1.0 - rate
    k0 = rho * rate
    k24 = k0 * (1.0 / 24.0)
    k6 = k0 * (1.0 / 6.0)
    half_b = 0.5 * b
    kt = k0 * t
    ktb = kt * b
    ktt = kt * t
    base = k0 * (1.0 - half_b + 0.5 * half_b * half_b)
    base1 = k0 * (0.5 - 0.5 * half_b)
    baseo = k0 * (1.0 - half_b)

    def even0(s):
        return (
            base
            + kt * (0.5 * (s - 3.0))
            + ktb * (0.25 * (5.0 - s))
            + ktt * ((s * s - 10.0 * s + 15.0) / 8.0)
        )

    emit(0, keep * rest + even0(0.0))
    for k in sums:
        s = 1.5 * k
        e0 = even0(s)
        e1 = base1 + kt * (0.25 * (s - 7.0))
        o1 = baseo + kt * (0.5 * (s - 5.0))
        for m, o in PAIRS:
            if SQUARES[m] != k:
                continue
            a = None
            for axis in range(3):
                v = SPEEDS[m][axis]
                if v == 0:
                    continue
                unit = w[axis]
                if a is None:
                    a = unit if v > 0 else -unit
                else:
                    a = a + unit if v > 0 else a - unit
            if size[k] != 1:
                a = float(size[k]) * a
            q = a * a
            even = e0 + q * (e1 + q * k24)
            odd = a * (o1 + q * k6)
            emit(m, keep * load(m) + (even + odd))
            emit(o, keep * load(o) + (even - odd))


def kernel(
    pop, rate, ext, g, r, zs, zr, y1s, y1r, y2s, y2r,
    in_sem, z_ss, z_rs, y1_ss, y1_rs, y2_ss, y2_rs, x_ss, x_rs,
):
    nx, ny, nz = pop.shape[1:]
    inner = nx - 4
    groups = [(0, 1), (nx - 1, 1), (1, 1), (nx - 2, 1), (2, inner)]
    loads = [
        pltpu.make_async_copy(
            pop.at[:, pl.ds(first, count)], g.at[:, pl.ds(first, count)], in_sem.at[n]
        )
        for n, (first, count) in enumerate(groups)
    ]
    loads.append(pltpu.make_async_copy(rate, r, in_sem.at[5]))

    around = []
    for axis in AXES:
        n = lax.axis_size(axis)
        me = lax.axis_index(axis)
        around.append(({axis: lax.rem(me + 1, n)}, {axis: lax.rem(me + n - 1, n)}))
    barrier = pltpu.get_barrier_semaphore()
    for pair in (around[1], around[0], around[2]):
        for target in pair:
            pl.semaphore_signal(barrier, inc=1, device_id=target, device_id_type=MESH)
    for n in (5, 0, 1, 2, 3, 4):
        loads[n].start()

    lane = lax.broadcasted_iota(jnp.int32, (ny, nz), 1)

    def layer_a(j):
        return (j % 2) * (nx - 1) + (j // 2) * (1 - 2 * (j % 2))

    def layer_b(j):
        return j + 2

    def rows_at(m):
        start = PY + SPEEDS[m][1]
        return pl.ds(start, ny)

    def edge_rows(sign, count):
        return pl.ds(PY + ny, count) if sign == 0 else pl.ds(PY - count, count)

    def home_rows(sign, count):
        return pl.ds(PY, count) if sign == 0 else pl.ds(PY + ny - count, count)

    def collide_chunk(chunk, layer, first, last, packed=None):
        def step(j, packed):
            x = layer(j)
            packed = list(packed)
            mine = [jnp.zeros((ny, nz), jnp.float32), jnp.zeros((ny, nz), jnp.float32)]
            slot = [{m: (s, c) for m, s, c in ZCOLS[d]} for d in (0, 1)]

            def emit(m, value):
                cx, cy, cz = SPEEDS[m]
                if cz:
                    d = 0 if cz > 0 else 1
                    start, count = slot[d][m]
                    shift = start + count if d == 0 else start
                    moved = pltpu.roll(value, shift, 1) if shift else value
                    mask = (lane >= start) & (lane < start + count)
                    mine[d] = jnp.where(mask, moved, mine[d])
                    value = pltpu.roll(value, cz % nz, 1)
                ext[m, PX + x + cx, rows_at(m), :] = value

            collide(lambda m: g[m, x], r[x], emit)
            for d in (0, 1):
                moved = pltpu.roll(mine[d], GROUP * j, 1)
                mask = (lane >= GROUP * j) & (lane < GROUP * j + GROUP)
                packed[d] = jnp.where(mask, moved, packed[d])
            for d in (0, 1):
                for m, start, count in Y1ROWS[d]:
                    y1s[chunk, d, j, pl.ds(start, count), :] = ext[
                        m, PX + x + SPEEDS[m][0], edge_rows(d, count), :
                    ]
            return tuple(packed)

        blank = jnp.zeros((ny, nz), jnp.float32)
        return lax.fori_loop(first, last, step, packed or (blank, blank))

    def pack_z(chunk, packed):
        for d in (0, 1):
            zs[chunk, d] = packed[d]

    def settle_z(chunk, layer, steps):
        def step(j, carry):
            x = layer(j)
            for d in (0, 1):
                back = lax.rem(nz - GROUP * j, nz)
                base = pltpu.roll(zr[chunk, d], back, 1)
                for m, start, count in ZCOLS[d]:
                    shift = start if d == 0 else start + count
                    moved = pltpu.roll(base, nz - shift, 1) if shift else base
                    mask = lane < count if d == 0 else lane >= nz - count
                    where = (m, PX + x + SPEEDS[m][0], rows_at(m), slice(None))
                    ext[where] = jnp.where(mask, moved, ext[where])
            for d in (0, 1):
                for m, start, count in Y2ROWS[d]:
                    y2s[chunk, d, j, pl.ds(start, count), :] = ext[
                        m, PX + x + SPEEDS[m][0], edge_rows(d, count), :
                    ]
            return carry

        lax.fori_loop(0, steps, step, 0)

    def settle_y(chunk, layer, steps, table, received):
        def step(j, carry):
            x = layer(j)
            for d in (0, 1):
                for m, start, count in table[d]:
                    ext[m, PX + x + SPEEDS[m][0], home_rows(d, count), :] = received[
                        chunk, d, j, pl.ds(start, count), :
                    ]
            return carry

        lax.fori_loop(0, steps, step, 0)

    def send_all(axis, chunk, src, dst, ss, rs):
        copies = []
        for d in (0, 1):
            copies.append(
                pltpu.make_async_remote_copy(
                    src_ref=src.at[chunk, d],
                    dst_ref=dst.at[chunk, d],
                    send_sem=ss.at[chunk, d],
                    recv_sem=rs.at[chunk, d],
                    device_id=around[axis][d],
                    device_id_type=MESH,
                )
            )
        for copy in copies:
            copy.start()
        return copies

    xs = []
    early = [(8, ny - 8), (0, ny - 8)]
    late = [(0, 8), (ny - 8, 8)]

    def send_x(pair, rows=None):
        start, count = rows or (0, ny)
        for d in (0, 1):
            first, members, layers = pair[d]
            n = len(xs)
            out_at = PX + nx if d == 0 else PX - layers
            in_at = PX if d == 0 else PX + nx - layers
            which, rows = pl.ds(first, members), pl.ds(PY + start, count)
            copy = pltpu.make_async_remote_copy(
                src_ref=ext.at[which, pl.ds(out_at, layers), rows],
                dst_ref=ext.at[which, pl.ds(in_at, layers), rows],
                send_sem=x_ss.at[n],
                recv_sem=x_rs.at[n],
                device_id=around[0][d],
                device_id_type=MESH,
            )
            copy.start()
            xs.append(copy)

    for n in (5, 0, 1):
        loads[n].wait()
    packed = collide_chunk(0, layer_a, 0, 2)
    loads[2].wait()
    loads[3].wait()
    pack_z(0, collide_chunk(0, layer_a, 2, 4, packed))
    pl.semaphore_wait(barrier, 6)
    send_x(XPURE[0])
    send_x(XPURE[1])
    z_a = send_all(2, 0, zs, zr, z_ss, z_rs)
    y1_a = send_all(1, 0, y1s, y1r, y1_ss, y1_rs)
    for n in (0, 1):
        send_x(XY[n], early[n])
    loads[4].wait()
    pack_z(1, collide_chunk(1, layer_b, 0, inner))
    z_b = send_all(2, 1, zs, zr, z_ss, z_rs)
    y1_b = send_all(1, 1, y1s, y1r, y1_ss, y1_rs)
    send_x(XPURE[2])

    for copy in z_a:
        copy.wait_recv()
    settle_z(0, layer_a, 4)
    y2_a = send_all(1, 0, y2s, y2r, y2_ss, y2_rs)
    send_x(XZ)
    for n in (0, 1):
        send_x(XYZ[n], early[n])
    for copy in y1_a:
        copy.wait_recv()
    settle_y(0, layer_a, 4, Y1ROWS, y1r)
    for n in (0, 1):
        send_x(XY[n], late[n])
    for copy in z_b:
        copy.wait_recv()
    settle_z(1, layer_b, inner)
    y2_b = send_all(1, 1, y2s, y2r, y2_ss, y2_rs)
    for copy in y2_a:
        copy.wait_recv()
    settle_y(0, layer_a, 4, Y2ROWS, y2r)
    for n in (0, 1):
        send_x(XYZ[n], late[n])
    for copy in y1_b:
        copy.wait_recv()
    settle_y(1, layer_b, inner, Y1ROWS, y1r)
    for copy in y2_b:
        copy.wait_recv()
    settle_y(1, layer_b, inner, Y2ROWS, y2r)
    for copy in xs:
        copy.wait_recv()
    for copy in z_a + z_b + y1_a + y1_b + y2_a + y2_b + xs:
        copy.wait_send()


def crop(ext, out, sem):
    nx, ny = out.shape[1:3]
    parts = 3
    share = Q // parts
    copies = [
        pltpu.make_async_copy(
            ext.at[pl.ds(n * share, share), pl.ds(PX, nx), pl.ds(PY, ny)],
            out.at[pl.ds(n * share, share)],
            sem.at[n],
        )
        for n in range(parts)
    ]
    for copy in copies:
        copy.start()
    for copy in copies:
        copy.wait()


def per_device(populations, relax):
    nx, ny, nz = relax.shape
    steps = max(4, nx - 4)
    shape = (Q, nx + 2 * PX, ny + 2 * PY, nz)
    f32 = jnp.float32
    dma = pltpu.SemaphoreType.DMA
    any_space = pl.BlockSpec(memory_space=pl.ANY)
    room = 67043328 - 4 * math.prod(shape) - 32768
    ext = pl.pallas_call(
        kernel,
        out_shape=pltpu.VMEM(shape, f32),
        in_specs=[pl.BlockSpec(memory_space=pltpu.HBM)] * 2,
        out_specs=pl.BlockSpec(memory_space=pltpu.VMEM),
        scratch_shapes=[
            pltpu.VMEM((Q, nx, ny, nz), f32),
            pltpu.VMEM((nx, ny, nz), f32),
            pltpu.VMEM((2, 2, ny, nz), f32),
            pltpu.VMEM((2, 2, ny, nz), f32),
            pltpu.VMEM((2, 2, steps, Y1SIZE, nz), f32),
            pltpu.VMEM((2, 2, steps, Y1SIZE, nz), f32),
            pltpu.VMEM((2, 2, steps, Y2SIZE, nz), f32),
            pltpu.VMEM((2, 2, steps, Y2SIZE, nz), f32),
            dma((6,)),
            dma((2, 2)), dma((2, 2)),
            dma((2, 2)), dma((2, 2)),
            dma((2, 2)), dma((2, 2)),
            dma((24,)), dma((24,)),
        ],
        compiler_params=pltpu.CompilerParams(
            collective_id=0, has_side_effects=True, vmem_limit_bytes=room
        ),
    )(populations, relax)
    return pl.pallas_call(
        crop,
        out_shape=jax.ShapeDtypeStruct((Q, nx, ny, nz), f32),
        in_specs=[any_space],
        out_specs=any_space,
        scratch_shapes=[dma((3,))],
        compiler_params=pltpu.CompilerParams(vmem_limit_bytes=2**20),
    )(ext)


def solution(mesh):
    return jax.shard_map(
        per_device,
        mesh=mesh,
        in_specs=(P(None, "gx", "gy", "gz"), P("gx", "gy", "gz")),
        out_specs=P(None, "gx", "gy", "gz"),
        check_vma=False,
    )
```
